32 devices in a mesh: tm: 16 (over z, x, core), grp: 2 (over y).
Axes of the slice: x: 2, y: 2, z: 4, core: 2. Of those that a mesh axis runs over, the one named last changes fastest.
Arguments:
- residual: float32 [16, 2, 3072], P('tm', 'grp'), may hold values from -6 to 6
- weight: float32 [16, 2, 3072], P('tm', 'grp'), may hold values from 0.25 to 4
- source_part: float32 [5, 16, 2, 3072], P(None, 'tm', 'grp'), may hold values from -2.5 to 2.5
- source_index: int32 [16, 2, 3072], P('tm', 'grp'), may hold values from 0 to 4095
- source_delta: float32 [5, 16, 4096], P(None, 'tm'), may hold values from -6 to 6
- attitude_part: float32 [3, 16, 2, 3072], P(None, 'tm', 'grp'), may hold values from -6 to 6
- spline_phase: float32 [16, 2, 3072], P('tm', 'grp'), may hold values from 0 to 1
- knot_index: int32 [16, 2, 3072], P('tm', 'grp'), may hold values from 0 to 1535, as said below
- calib_part: float32 [6, 16, 2, 3072], P(None, 'tm', 'grp'), may hold values from -6 to 6
- calib_index: int32 [16, 2, 3072], P('tm', 'grp'), may hold values from 0 to 2047
- global_part: float32 [4, 16, 2, 3072], P(None, 'tm', 'grp'), may hold values from -6 to 6
Outputs:
- residual_new: float32 [16, 2, 3072], P('tm', 'grp')
- attitude_step: float32 [3, 1536], P(None, 'tm')
- calib_step: float32 [6, 2048], replicated
- global_step: float32 [4], replicated
The draws below stay inside these ranges and needn't reach their ends.
Inputs may be any that keep to these rules, and one draw needn't show every extreme that they name: `knot_index`: observation r of interval t (in any group) lies in knot interval t * 96 + 4 * (r // 128) + j for some j in 0 .. 3.
All inputs are finite; a program needn't handle non-finite values.
Results may differ from the reference program's by a relative error of at most 0.00012.
Values sent between devices are 32-bit elements; how exact they have to be, the bound alone decides.
A program may use at most 128 MiB of HBM per device.

```python
import math
import jax
import jax.numpy as jnp
from jax import lax

ROWS_DEV = 3072
TILE = 128
KPT = 4
SRC_DEV = 4096
UNITS = 2048
CPAR = 6
GPAR = 4
ATT_SWEEPS = 4
ND = 96
INTERVALS = 16
GROUPS = 2


def draw_knot_index(key, part):
    within = jax.random.randint(key, (INTERVALS, GROUPS, ROWS_DEV), 0, KPT, dtype=jnp.int32)
    tile_base = KPT * (jnp.arange(ROWS_DEV, dtype=jnp.int32) // TILE)
    interval_base = jnp.arange(INTERVALS, dtype=jnp.int32) * ND
    return (interval_base[:, None, None] + tile_base[None, None, :] + within).astype(jnp.int32)


def with_ends(drawn, rng, low, top_value):
    longest = drawn.shape.index(max(drawn.shape))
    spots = []
    for shift in (0, 1):
        where = [jax.random.randint(jax.random.fold_in(rng, axis), (), 0, length) for axis, length in enumerate(drawn.shape)]
        where[longest] = (where[longest] + shift) % drawn.shape[longest]
        spots.append(tuple(where))
    return drawn.at[spots[0]].set(low).at[spots[1]].set(top_value)


def level_of(stream_key, shape, cuts, least, top_value):
    loudness, own = 1.0, jax.random.fold_in(stream_key, 6)
    for dim, parts in cuts:
        steps = jnp.exp(jax.random.uniform(jax.random.fold_in(own, dim), (parts,), jnp.float32, least / len(cuts), top_value / len(cuts)))
        loudness = loudness * jnp.repeat(steps, shape[dim] // parts).reshape([-1 if axis == dim else 1 for axis in range(len(shape))])
    return loudness


def scatter_about(own_key, dims, scale, limit, split=(), kind=jnp.bfloat16):
    array = scale * jax.random.normal(own_key, dims, jnp.float32)
    if split:
        array = array * level_of(own_key, dims, split, -0.22, 0.18)
    return jnp.clip(array, -limit, limit).astype(kind)


def setup_inputs(seed: int = 0) -> dict:
    streams_of = jax.random.split(jax.random.key(seed), 12)
    return {
        "residual": scatter_about(streams_of[0], (INTERVALS, GROUPS, ROWS_DEV), 1.0, 6.0, ((0, 16), (1, 2)), jnp.float32),
        "weight": jnp.clip(jnp.exp(math.log(4.0) - 2.7725887 * jax.random.uniform(streams_of[1], (INTERVALS, GROUPS, ROWS_DEV), jnp.float32) ** level_of(streams_of[1], (INTERVALS, GROUPS, ROWS_DEV), ((0, 16), (1, 2)), -0.2, 0.2)), 0.25, 4.0),
        "source_part": scatter_about(streams_of[2], (5, INTERVALS, GROUPS, ROWS_DEV), 5 ** -0.5, 2.5, ((1, 16), (2, 2)), jnp.float32),
        "source_index": with_ends(jax.random.randint(streams_of[3], (INTERVALS, GROUPS, ROWS_DEV), 0, SRC_DEV), jax.random.fold_in(streams_of[3], 1), 0, SRC_DEV - 1).astype(jnp.int32),
        "source_delta": scatter_about(streams_of[4], (5, INTERVALS, SRC_DEV), 1.0, 6.0, ((1, 16),), jnp.float32),
        "attitude_part": scatter_about(streams_of[5], (3, INTERVALS, GROUPS, ROWS_DEV), 1.0, 6.0, ((1, 16), (2, 2)), jnp.float32),
        "spline_phase": jnp.clip(1.0 * jax.random.uniform(streams_of[6], (INTERVALS, GROUPS, ROWS_DEV), jnp.float32) ** level_of(streams_of[6], (INTERVALS, GROUPS, ROWS_DEV), ((0, 16), (1, 2)), -0.2, 0.2), 0.0, 1.0),
        "knot_index": draw_knot_index(jax.random.fold_in(streams_of[11], 71), 0),
        "calib_part": scatter_about(streams_of[8], (CPAR, INTERVALS, GROUPS, ROWS_DEV), 1.0, 6.0, ((1, 16), (2, 2)), jnp.float32),
        "calib_index": with_ends(jax.random.randint(streams_of[9], (INTERVALS, GROUPS, ROWS_DEV), 0, UNITS), jax.random.fold_in(streams_of[9], 1), 0, UNITS - 1).astype(jnp.int32),
        "global_part": scatter_about(streams_of[10], (GPAR, INTERVALS, GROUPS, ROWS_DEV), 1.0, 6.0, ((1, 16), (2, 2)), jnp.float32),
    }


OMEGA = 0.6
RIDGE = 1.0

def spline_basis(phase):
    inverse = 1.0 - phase
    square = phase * phase
    cubed = square * phase
    return [inverse * inverse * inverse / 6.0, (3.0 * cubed - 6.0 * square + 4.0) / 6.0, (-3.0 * cubed + 3.0 * square + 3.0 * phase + 1.0) / 6.0, cubed / 6.0]

def cholesky_lists(matrix, extent):
    lower_tri = [[None for column in range(extent)] for target in range(extent)]
    for column in range(extent):
        pivot_sq = matrix[column][column]
        for inner_k in range(column):
            pivot_sq = pivot_sq - lower_tri[column][inner_k] * lower_tri[column][inner_k]
        pivot_val = jnp.sqrt(pivot_sq)
        lower_tri[column][column] = pivot_val
        for target in range(column + 1, extent):
            entry_val = matrix[target][column]
            for inner_k in range(column):
                entry_val = entry_val - lower_tri[target][inner_k] * lower_tri[column][inner_k]
            lower_tri[target][column] = entry_val / pivot_val
    return lower_tri

def solve_lower(lower_tri, vector):
    result = []
    for target in range(len(vector)):
        running = vector[target]
        for inner_k in range(target):
            running = running - lower_tri[target][inner_k] * result[inner_k]
        result.append(running / lower_tri[target][target])
    return result

def solve_upper(lower_tri, vector):
    extent = len(vector)
    result = [None for target in range(extent)]
    for target in reversed(range(extent)):
        running = vector[target]
        for inner_k in range(target + 1, extent):
            running = running - lower_tri[inner_k][target] * result[inner_k]
        result[target] = running / lower_tri[target][target]
    return result

def upper_pairs(extent):
    return [(first, second) for first in range(extent) for second in range(first, extent)]

def symmetric_lists(upper_values, extent):
    matrix = [[None for second in range(extent)] for first in range(extent)]
    for position, index_pair in enumerate(upper_pairs(extent)):
        first, second = index_pair
        value_now = upper_values[position] + (RIDGE if first == second else 0.0)
        matrix[first][second] = value_now
        matrix[second][first] = value_now
    return matrix

def solve_blocks(upper_values, rhs_values, extent):
    lower_tri = cholesky_lists(symmetric_lists(upper_values, extent), extent)
    whitened = solve_lower(lower_tri, rhs_values)
    solution = solve_upper(lower_tri, whitened)
    return (jnp.stack(whitened), jnp.stack(solution))

def apply_band(band_own, band_left, padded):
    extent = band_own.shape[-1]
    result = padded[:, 3:3 + extent]
    for offset in range(4):
        ahead_x = padded[:, 3 + offset:3 + offset + extent]
        result = result + lax.optimization_barrier(jnp.sum(band_own[offset] * ahead_x[None, :, :], axis=1))
    for offset in range(1, 4):
        behind = padded[:, 3 - offset:3 - offset + extent]
        blocks = band_left[offset][:, :, 3 - offset:3 - offset + extent]
        result = result + lax.optimization_barrier(jnp.sum(blocks * behind[:, None, :], axis=0))
    return result

def node_sweeps(band_own, band_left, rhs_att, extend):
    diagonal = [[band_own[0][first, second] + (RIDGE if first == second else 0.0) for second in range(3)] for first in range(3)]
    lower_tri = cholesky_lists(diagonal, 3)

    def precondition(vector):
        return jnp.stack(solve_upper(lower_tri, solve_lower(lower_tri, [vector[axis_k] for axis_k in range(3)])))
    answer = OMEGA * precondition(rhs_att)
    for sweep_no in range(1, ATT_SWEEPS):
        padded = extend(answer)
        answer = answer + OMEGA * precondition(rhs_att - apply_band(band_own, band_left, padded))
    padded = extend(answer)
    scaled = jnp.stack([sum((lower_tri[inner_k][target] * answer[inner_k] for inner_k in range(target, 3))) for target in range(3)])
    return (answer, padded, scaled)

def node_features(vectors, weights, first_res, basis_no):
    term_list = []
    for offset in range(4 - basis_no):
        for first in range(3):
            for second in range(3):
                term_list.append(weights * vectors[basis_no][first] * vectors[basis_no + offset][second])
    for first in range(3):
        term_list.append(weights * vectors[basis_no][first] * first_res)
    return jnp.stack(term_list)

def spread_terms(stacked, basis_no):
    band_rows = (4 - basis_no) * 9
    filler = jnp.zeros((basis_no * 9,) + stacked.shape[1:], jnp.float32)
    return jnp.concatenate([stacked[:band_rows], filler, stacked[band_rows:]], axis=0)

def unit_matrix_terms(rows_part, weights):
    return [weights * rows_part[first] * rows_part[second] for first, second in upper_pairs(rows_part.shape[0])]

def rhs_terms(rows_part, weights, resid_now):
    return [weights * rows_part[first] * resid_now for first in range(rows_part.shape[0])]

def reference(residual, weight, source_part, source_index, source_delta, attitude_part, spline_phase, knot_index, calib_part, calib_index, global_part):
    nodes_dev = ND
    interval_ids = jnp.arange(INTERVALS, dtype=jnp.int32)

    def interval_rows(index_t):
        weights = weight[index_t].reshape(-1)
        source_rows = source_part[:, index_t].reshape(5, -1)
        picked = jnp.take(source_delta[:, index_t], source_index[index_t].reshape(-1), axis=1)
        first_res = residual[index_t].reshape(-1) - lax.optimization_barrier(jnp.sum(source_rows * picked, axis=0))
        basis_list = spline_basis(spline_phase[index_t].reshape(-1))
        att_rows = attitude_part[:, index_t].reshape(3, -1)
        vectors = [basis_val[None, :] * att_rows for basis_val in basis_list]
        local_knot = knot_index[index_t].reshape(-1) - index_t * nodes_dev
        return (weights, first_res, vectors, local_knot)

    def first_pass(index_t):
        weights, first_res, vectors, local_knot = interval_rows(index_t)
        local_sums = jnp.zeros((39, nodes_dev + 3), jnp.float32)
        for basis_no in range(4):
            stacked = node_features(vectors, weights, first_res, basis_no)
            binned = jax.ops.segment_sum(stacked.T, local_knot + basis_no, num_segments=nodes_dev + 3).T
            local_sums = local_sums + spread_terms(binned, basis_no)
        return local_sums
    local_all = lax.map(first_pass, interval_ids)
    spill_out = local_all[:, :, nodes_dev:]
    shifted = jnp.concatenate([jnp.zeros((1, 39, 3), jnp.float32), spill_out[:-1]], axis=0)
    main_part = local_all[:, :, :nodes_dev]
    main_part = jnp.concatenate([main_part[:, :, :3] + shifted, main_part[:, :, 3:]], axis=2)
    totals = jnp.transpose(main_part, (1, 0, 2)).reshape(39, INTERVALS * nodes_dev)
    band_own = totals[:36].reshape(4, 3, 3, -1)
    band_left = jnp.concatenate([jnp.zeros((4, 3, 3, 3), jnp.float32), band_own], axis=3)

    def extend(vector):
        return jnp.pad(vector, ((0, 0), (3, 3)))
    answer, padded, attitude_step = node_sweeps(band_own, band_left, totals[36:], extend)
    node_values = padded[:, 3:]

    def second_pass(index_t):
        weights, first_res, vectors, local_knot = interval_rows(index_t)
        global_knot = knot_index[index_t].reshape(-1)
        second_res = first_res
        for basis_no in range(4):
            picked_nodes = jnp.take(node_values, global_knot + basis_no, axis=1)
            second_res = second_res - lax.optimization_barrier(jnp.sum(vectors[basis_no] * picked_nodes, axis=0))
        calib_rows = calib_part[:, index_t].reshape(CPAR, -1)
        global_rows = global_part[:, index_t].reshape(GPAR, -1)
        unit_ids = calib_index[index_t].reshape(-1)
        features = jnp.stack(unit_matrix_terms(calib_rows, weights) + rhs_terms(calib_rows, weights, second_res))
        unit_terms = jax.ops.segment_sum(features.T, unit_ids, num_segments=UNITS).T
        global_terms = jnp.stack([jnp.sum(term_row) for term_row in unit_matrix_terms(global_rows, weights) + rhs_terms(global_rows, weights, second_res)])
        return (second_res, unit_terms, global_terms)
    second_all, unit_all, global_all = lax.map(second_pass, interval_ids)
    unit_total = lax.optimization_barrier(jnp.sum(unit_all, axis=0))
    global_total = lax.optimization_barrier(jnp.sum(global_all, axis=0))
    pair_count = CPAR * (CPAR + 1) // 2
    pair_global = GPAR * (GPAR + 1) // 2
    calib_step, calib_solution = solve_blocks(unit_total[:pair_count], [unit_total[pair_count + first] for first in range(CPAR)], CPAR)
    global_step, global_solution = solve_blocks(global_total[:pair_global], [global_total[pair_global + first] for first in range(GPAR)], GPAR)

    def third_pass(carried):
        index_t, second_res = carried
        calib_rows = calib_part[:, index_t].reshape(CPAR, -1)
        global_rows = global_part[:, index_t].reshape(GPAR, -1)
        unit_values = jnp.take(calib_solution, calib_index[index_t].reshape(-1), axis=1)
        final_res = second_res - lax.optimization_barrier(jnp.sum(calib_rows * unit_values, axis=0)) - lax.optimization_barrier(jnp.sum(global_rows * global_solution[:, None], axis=0))
        return final_res.reshape(GROUPS, ROWS_DEV)
    residual_new = lax.map(third_pass, (interval_ids, second_all))
    return (residual_new, attitude_step, calib_step, global_step)
```

```python
import functools

import jax
import jax.numpy as jnp
from jax import lax
from jax.experimental import pallas as pl
from jax.experimental.pallas import tpu as pltpu
from jax.sharding import PartitionSpec as P

TILE = 128
KPT = 4
UNITS = 2048
CPAR = 6
GPAR = 4
ATT_SWEEPS = 4

OMEGA = 0.6
RIDGE = 1.0
LANES = 128
LOW = 256
HALO = 3 * ATT_SWEEPS
MESH = pl.DeviceIdType.MESH
F32 = jnp.float32
BF16 = jnp.bfloat16

ATT_ROWS = 72
UNIT_ROWS = 24
NORMAL_ROWS = 32


def pairs_of(extent):
    return [(a, b) for a in range(extent) for b in range(a, extent)]


def lane_pick(table, index):
    return lax.gather(
        table,
        index[..., None],
        lax.GatherDimensionNumbers(
            offset_dims=(),
            collapsed_slice_dims=(1,),
            start_index_map=(1,),
            operand_batching_dims=(0,),
            start_indices_batching_dims=(0,),
        ),
        (1, 1),
        mode=lax.GatherScatterMode.PROMISE_IN_BOUNDS,
    )


def spline_basis(phase):
    inverse = 1.0 - phase
    square = phase * phase
    cubed = square * phase
    return [
        inverse * inverse * inverse / 6.0,
        (3.0 * cubed - 6.0 * square + 4.0) / 6.0,
        (-3.0 * cubed + 3.0 * square + 3.0 * phase + 1.0) / 6.0,
        cubed / 6.0,
    ]


def cholesky_lists(matrix, extent):
    lower = [[None] * extent for _ in range(extent)]
    inverse = [None] * extent
    for column in range(extent):
        pivot = matrix[column][column]
        for k in range(column):
            pivot = pivot - lower[column][k] * lower[column][k]
        root = jnp.sqrt(pivot)
        lower[column][column] = root
        inverse[column] = 1.0 / root
        for row in range(column + 1, extent):
            entry = matrix[row][column]
            for k in range(column):
                entry = entry - lower[row][k] * lower[column][k]
            lower[row][column] = entry * inverse[column]
    return lower, inverse


def solve_lower(lower, inverse, vector):
    result = []
    for row in range(len(vector)):
        running = vector[row]
        for k in range(row):
            running = running - lower[row][k] * result[k]
        result.append(running * inverse[row])
    return result


def solve_upper(lower, inverse, vector):
    extent = len(vector)
    result = [None] * extent
    for row in reversed(range(extent)):
        running = vector[row]
        for k in range(row + 1, extent):
            running = running - lower[k][row] * result[k]
        result[row] = running * inverse[row]
    return result


def symmetric(upper, extent):
    matrix = [[None] * extent for _ in range(extent)]
    for position, (a, b) in enumerate(pairs_of(extent)):
        value = upper[position] + (RIDGE if a == b else 0.0)
        matrix[a][b] = value
        matrix[b][a] = value
    return matrix


def split_three(value):
    first = value.astype(BF16).astype(F32)
    rest = value - first
    second = rest.astype(BF16).astype(F32)
    third = (rest - second).astype(BF16).astype(F32)
    return [first, second, third]


def dot_nt(left, right):
    return lax.dot_general(
        left, right, (((1,), (1,)), ((), ())), preferred_element_type=F32
    )


def two_tiles(ref, tile, rows, tiles):
    return jnp.concatenate(
        [ref[pl.ds(tile, rows, stride=tiles), :], ref[pl.ds(tile + 1, rows, stride=tiles), :]],
        axis=1,
    )


def two_rows(ref, tile):
    return jnp.concatenate([ref[pl.ds(tile, 1), :], ref[pl.ds(tile + 1, 1), :]], axis=1)


def one_hot(row, extent):
    spots = lax.broadcasted_iota(jnp.int32, (extent, row.shape[1]), 0)
    return jnp.where(spots == row, 1.0, 0.0).astype(BF16)


def by_high(part, high):
    return jnp.concatenate(
        [jnp.where(high == h, part, 0.0) for h in range(UNITS // LOW)], axis=0
    )


def block_pieces(blocks):
    width = UNITS // blocks
    for piece in range(UNITS // LANES):
        unit = piece * LANES
        yield unit // width, unit % width, unit // LOW, unit % LOW


def first_kernel(
    blocks, res_ref, w_ref, sp_ref, si_ref, sd_ref, ap_ref, ph_ref, kn_ref, cp_ref, ci_ref,
    gp_ref, first_ref, normal_ref, mats_ref, att, cal, acc_att, acc_cal,
):
    tiles = res_ref.shape[0]
    weights = w_ref[...]
    sources = si_ref[...]
    high, low = lax.shift_right_logical(sources, 7), lax.bitwise_and(sources, 127)
    picked = [jnp.zeros((tiles, LANES), F32) for _ in range(5)]
    for row in range(sd_ref.shape[1]):
        here = high == row
        for c in range(5):
            table = jnp.broadcast_to(sd_ref[c, row : row + 1, :], (tiles, LANES))
            picked[c] = jnp.where(here, lane_pick(table, low), picked[c])
    total = sp_ref[0] * picked[0]
    for c in range(1, 5):
        total = total + sp_ref[c] * picked[c]
    first = res_ref[...] - total
    first_ref[...] = first
    basis = spline_basis(ph_ref[...])
    axes = [ap_ref[c] for c in range(3)]
    products = [weights * axes[a] * axes[b] for a, b in pairs_of(3)]
    rights = [weights * axes[a] * first for a in range(3)]
    place = 0
    for i in range(4):
        for d in range(4 - i):
            both = basis[i] * basis[i + d]
            for product in products:
                att[place * tiles : (place + 1) * tiles, :] = both * product
                place += 1
    for i in range(4):
        for right in rights:
            att[place * tiles : (place + 1) * tiles, :] = basis[i] * right
            place += 1
    place = 0
    for a, b in pairs_of(CPAR):
        cal[place * tiles : (place + 1) * tiles, :] = weights * cp_ref[a] * cp_ref[b]
        place += 1
    cal[place * tiles :, :] = jnp.zeros(((UNIT_ROWS - place) * tiles, LANES), F32)
    global_rows = [
        jnp.sum(weights * gp_ref[a] * gp_ref[b], axis=0, keepdims=True)
        for a, b in pairs_of(GPAR)
    ]
    acc_att[...] = jnp.zeros_like(acc_att)
    acc_cal[...] = jnp.zeros_like(acc_cal)
    base = lax.axis_index("tm") * (tiles * KPT)

    def step(no, carry):
        tile = no * 2
        knots = two_rows(kn_ref, tile) - base
        nodes = one_hot(knots, LANES)
        part = acc_att[...]
        for piece in split_three(two_tiles(att, tile, ATT_ROWS, tiles)):
            part = part + dot_nt(piece.astype(BF16), nodes)
        acc_att[...] = part
        units = two_rows(ci_ref, tile)
        upper, lower = lax.shift_right_logical(units, 8), lax.bitwise_and(units, 255)
        spots = one_hot(lower, LOW)
        part = acc_cal[...]
        for piece in split_three(two_tiles(cal, tile, UNIT_ROWS, tiles)):
            part = part + dot_nt(by_high(piece, upper).astype(BF16), spots)
        acc_cal[...] = part
        return carry

    lax.fori_loop(0, tiles // 2, step, 0, unroll=2)
    band = [None] * 5
    place = 0
    for i in range(4):
        for d in list(range(4 - i)):
            rows = acc_att[place : place + 6, :]
            rows = pltpu.roll(rows, i, 1) if i else rows
            band[d] = rows if band[d] is None else band[d] + rows
            place += 6
    for i in range(4):
        rows = acc_att[place : place + 3, :]
        rows = pltpu.roll(rows, i, 1) if i else rows
        band[4] = rows if band[4] is None else band[4] + rows
        place += 3
    for d in range(4):
        normal_ref[d * 6 : (d + 1) * 6, :] = band[d]
    normal_ref[24:27, :] = band[4]
    normal_ref[27:, :] = jnp.zeros((NORMAL_ROWS - 27, LANES), F32)
    mats_ref[...] = jnp.zeros_like(mats_ref)
    for block, at, h, start in block_pieces(blocks):
        mats_ref[block, 0:21, at : at + LANES] = acc_cal[
            h * UNIT_ROWS : h * UNIT_ROWS + 21, start : start + LANES
        ]
        if at == 0:
            for no, row in enumerate(global_rows):
                mats_ref[block, 21 + no : 22 + no, 0:LANES] = row


def attitude_kernel(
    shape, nodes_dev, normal_ref, mats_ref, x_ref, total_ref,
    near, mine, whole, near_s, near_r, mine_s, mine_r, whole_s, whole_r,
):
    count, groups, blocks = shape
    t, g = lax.axis_index("tm"), lax.axis_index("grp")
    has_before, has_after = t > 0, t < count - 1

    def peer_tm(k):
        return lax.rem(t + k, count)

    def peer_grp(k):
        return lax.rem(g + k, groups)

    barrier = pltpu.get_barrier_semaphore()

    def greet(where):
        pl.semaphore_signal(barrier, inc=1, device_id=where, device_id_type=MESH)

    lax.fori_loop(1, count, lambda k, c: (greet({"tm": peer_tm(k), "grp": g}), c)[1], 0)
    for k in range(1, groups):
        greet({"tm": t, "grp": peer_grp(k)})
        greet({"tm": peer_tm(1), "grp": peer_grp(k)})
        greet({"tm": peer_tm(count - 1), "grp": peer_grp(k)})
    pl.semaphore_wait(barrier, count - 1 + 3 * (groups - 1))

    def near_copy(offset, k):
        slot = (1 - offset) * groups + g
        return pltpu.make_async_remote_copy(
            src_ref=normal_ref,
            dst_ref=near.at[slot],
            send_sem=near_s.at[(offset + 1) * groups + k],
            recv_sem=near_r.at[slot],
            device_id={"tm": t + offset, "grp": peer_grp(k)},
            device_id_type=MESH,
        )

    def near_arrival(offset, k):
        slot = (offset + 1) * groups + peer_grp(k)
        return pltpu.make_async_remote_copy(
            src_ref=normal_ref,
            dst_ref=near.at[slot],
            send_sem=near_s.at[(offset + 1) * groups + k],
            recv_sem=near_r.at[slot],
            device_id={"tm": t + offset, "grp": peer_grp(k)},
            device_id_type=MESH,
        )

    def each_near(do):
        for k in range(1, groups):
            do(0, k)

        @pl.when(has_before)
        def _():
            for k in range(groups):
                do(-1, k)

        @pl.when(has_after)
        def _():
            for k in range(groups):
                do(1, k)

    each_near(lambda offset, k: near_copy(offset, k).start())

    def whole_copy(k):
        p = peer_tm(k)
        return pltpu.make_async_remote_copy(
            src_ref=mats_ref.at[lax.rem(p, blocks)],
            dst_ref=whole.at[t],
            send_sem=whole_s.at[k],
            recv_sem=whole_r.at[t],
            device_id={"tm": p, "grp": g},
            device_id_type=MESH,
        )

    def whole_arrival(k):
        p = peer_tm(k)
        return pltpu.make_async_remote_copy(
            src_ref=mats_ref.at[lax.rem(p, blocks)],
            dst_ref=whole.at[p],
            send_sem=whole_s.at[k],
            recv_sem=whole_r.at[p],
            device_id={"tm": p, "grp": g},
            device_id_type=MESH,
        )

    lax.fori_loop(1, count, lambda k, c: (whole_copy(k).start(), c)[1], 0)
    whole[t] = mats_ref[lax.rem(t, blocks)]
    near[groups + g] = normal_ref[...]

    @pl.when(jnp.logical_not(has_before))
    def _():
        near[0:groups] = jnp.zeros((groups, NORMAL_ROWS, LANES), F32)

    @pl.when(jnp.logical_not(has_after))
    def _():
        near[2 * groups :] = jnp.zeros((groups, NORMAL_ROWS, LANES), F32)

    each_near(lambda offset, k: near_arrival(offset, k).wait_recv())
    sums = []
    for s in range(3):
        part = near[s * groups]
        for q in range(1, groups):
            part = part + near[s * groups + q]
        sums.append(part)
    lane = lax.broadcasted_iota(jnp.int32, (NORMAL_ROWS, LANES), 1)
    before = pltpu.roll(sums[0], (HALO - nodes_dev) % LANES, 1)
    own = pltpu.roll(sums[1], HALO, 1)
    after = pltpu.roll(sums[2], (HALO + nodes_dev) % LANES, 1)
    end = nodes_dev + HALO
    normals = (
        own
        + jnp.where((lane >= 3) & (lane < HALO + 3), before, 0.0)
        + jnp.where((lane >= end) & (lane < end + HALO), after, 0.0)
    )
    spot = lax.broadcasted_iota(jnp.int32, (1, LANES), 1)
    exists = (spot >= jnp.where(has_before, 0, HALO)) & (
        spot < jnp.where(has_after, LANES, end)
    )
    normals = jnp.where(exists, normals, 0.0)
    index = {}
    for position, (a, b) in enumerate(pairs_of(3)):
        index[a, b] = index[b, a] = position
    band = [[normals[d * 6 + p : d * 6 + p + 1, :] for p in range(6)] for d in range(4)]
    right = [normals[24 + c : 25 + c, :] for c in range(3)]
    lower, inverse = cholesky_lists(symmetric(band[0], 3), 3)

    def precondition(vector):
        return solve_upper(lower, inverse, solve_lower(lower, inverse, vector))

    x = [OMEGA * value for value in precondition(right)]
    for _ in range(1, ATT_SWEEPS):
        out = [right[c] - x[c] for c in range(3)]
        for d in range(4):
            ahead = [pltpu.roll(x[c], LANES - d, 1) for c in range(3)] if d else x
            for a in range(3):
                for b in range(3):
                    out[a] = out[a] - band[d][index[a, b]] * ahead[b]
        for d in range(1, 4):
            for a in range(3):
                term = band[d][index[a, 0]] * x[0]
                for b in range(1, 3):
                    term = term + band[d][index[a, b]] * x[b]
                out[a] = out[a] - pltpu.roll(term, d, 1)
        change = precondition(out)
        x = [jnp.where(exists, x[c] + OMEGA * change[c], 0.0) for c in range(3)]
    x_ref[...] = jnp.zeros_like(x_ref)
    for c in range(3):
        x_ref[c : c + 1, :] = x[c]
        scaled = lower[c][c] * x[c]
        for k in range(c + 1, 3):
            scaled = scaled + lower[k][c] * x[k]
        x_ref[3 + c : 4 + c, :] = pltpu.roll(scaled, LANES - HALO, 1)

    lax.fori_loop(1, count, lambda k, c: (whole_arrival(k).wait_recv(), c)[1], 0)
    mine[g] = lax.fori_loop(1, count, lambda k, c: c + whole[k], whole[0])

    def mine_copy(k):
        return pltpu.make_async_remote_copy(
            src_ref=mine.at[g],
            dst_ref=mine.at[g],
            send_sem=mine_s.at[k],
            recv_sem=mine_r.at[g],
            device_id={"tm": t, "grp": peer_grp(k)},
            device_id_type=MESH,
        )

    def mine_arrival(k):
        q = peer_grp(k)
        return pltpu.make_async_remote_copy(
            src_ref=mine.at[q],
            dst_ref=mine.at[q],
            send_sem=mine_s.at[k],
            recv_sem=mine_r.at[q],
            device_id={"tm": t, "grp": q},
            device_id_type=MESH,
        )

    for k in range(1, groups):
        mine_copy(k).start()
    for k in range(1, groups):
        mine_arrival(k).wait_recv()
    total = mine[0]
    for q in range(1, groups):
        total = total + mine[q]
    total_ref[...] = total
    for k in range(1, groups):
        mine_copy(k).wait_send()
    each_near(lambda offset, k: near_copy(offset, k).wait_send())
    lax.fori_loop(1, count, lambda k, c: (whole_copy(k).wait_send(), c)[1], 0)


def second_kernel(
    blocks, first_ref, x_ref, w_ref, ap_ref, ph_ref, kn_ref, cp_ref, ci_ref, gp_ref,
    second_ref, rhs_ref, step_ref, cal, acc,
):
    tiles = first_ref.shape[0]
    nodes_dev = tiles * KPT
    weights = w_ref[...]
    base = lax.axis_index("tm") * nodes_dev
    local = kn_ref[...] - base + HALO
    basis = spline_basis(ph_ref[...])
    tables = [jnp.broadcast_to(x_ref[c : c + 1, :], (tiles, LANES)) for c in range(3)]
    second = first_ref[...]
    for i in range(4):
        moved = ap_ref[0] * lane_pick(tables[0], local + i)
        for c in range(1, 3):
            moved = moved + ap_ref[c] * lane_pick(tables[c], local + i)
        second = second - basis[i] * moved
    second_ref[...] = second
    step_ref[...] = x_ref[3:6, 0:nodes_dev]
    weighted = weights * second
    for a in range(CPAR):
        cal[a * tiles : (a + 1) * tiles, :] = weighted * cp_ref[a]
    cal[CPAR * tiles :, :] = jnp.zeros(((8 - CPAR) * tiles, LANES), F32)
    sums = [jnp.sum(weighted * gp_ref[a], axis=0, keepdims=True) for a in range(GPAR)]
    acc[...] = jnp.zeros_like(acc)

    def step(no, carry):
        tile = no * 2
        units = two_rows(ci_ref, tile)
        upper, lower = lax.shift_right_logical(units, 8), lax.bitwise_and(units, 255)
        pieces = [by_high(p, upper) for p in split_three(two_tiles(cal, tile, 8, tiles))]
        lhs = jnp.concatenate(pieces, axis=0).astype(BF16)
        acc[...] = acc[...] + dot_nt(lhs, one_hot(lower, LOW))
        return carry

    lax.fori_loop(0, tiles // 2, step, 0, unroll=2)
    rows = 8 * (UNITS // LOW)
    total = acc[0:rows, :] + acc[rows : 2 * rows, :] + acc[2 * rows : 3 * rows, :]
    lane = lax.broadcasted_iota(jnp.int32, (1, LANES), 1)
    folded = [row + pltpu.roll(row, LANES // 2, 1) for row in sums]
    packed = [jnp.where(lane < LANES // 2, folded[2 * k], folded[2 * k + 1]) for k in range(2)]
    if rhs_ref.shape[2] > LANES:
        rhs_ref[...] = jnp.zeros_like(rhs_ref)
    for block, at, h, start in block_pieces(blocks):
        rhs_ref[block, 0:CPAR, at : at + LANES] = total[
            h * 8 : h * 8 + CPAR, start : start + LANES
        ]
        if at == 0:
            for k in range(2):
                rhs_ref[block, CPAR + k : CPAR + k + 1, 0:LANES] = packed[k]


def solve_kernel(
    shape, rhs_ref, total_ref, out_ref, glob_ref,
    whole, mine, ready, spread, whole_s, whole_r, mine_s, mine_r, spread_s, spread_r,
):
    count, groups, blocks = shape
    width = rhs_ref.shape[2]
    t, g = lax.axis_index("tm"), lax.axis_index("grp")
    block = lax.rem(t, blocks)
    family = t - block

    def peer_tm(k):
        return lax.rem(t + k, count)

    def peer_grp(k):
        return lax.rem(g + k, groups)

    barrier = pltpu.get_barrier_semaphore()

    def greet(where):
        pl.semaphore_signal(barrier, inc=1, device_id=where, device_id_type=MESH)

    lax.fori_loop(1, count, lambda k, c: (greet({"tm": peer_tm(k), "grp": g}), c)[1], 0)
    for k in range(1, groups):
        greet({"tm": t, "grp": peer_grp(k)})
    pl.semaphore_wait(barrier, count - 1 + groups - 1)

    def whole_copy(k, slot):
        p = peer_tm(k)
        return pltpu.make_async_remote_copy(
            src_ref=rhs_ref.at[lax.rem(p, blocks)],
            dst_ref=whole.at[slot],
            send_sem=whole_s.at[k],
            recv_sem=whole_r.at[slot],
            device_id={"tm": p, "grp": g},
            device_id_type=MESH,
        )

    lax.fori_loop(1, count, lambda k, c: (whole_copy(k, t).start(), c)[1], 0)
    whole[t] = rhs_ref[block]
    matrix = [total_ref[p : p + 1, :] for p in range(21)]
    lower, inverse = cholesky_lists(symmetric(matrix, CPAR), CPAR)
    upper_g = [
        jnp.broadcast_to(
            jnp.sum(total_ref[21 + p : 22 + p, 0:LANES], axis=1, keepdims=True), (1, LANES)
        )
        for p in range(10)
    ]
    lower_g, inverse_g = cholesky_lists(symmetric(upper_g, GPAR), GPAR)
    lax.fori_loop(1, count, lambda k, c: (whole_copy(k, peer_tm(k)).wait_recv(), c)[1], 0)
    mine[g] = lax.fori_loop(1, count, lambda k, c: c + whole[k], whole[0])

    def mine_copy(k, slot):
        return pltpu.make_async_remote_copy(
            src_ref=mine.at[slot],
            dst_ref=mine.at[slot],
            send_sem=mine_s.at[k],
            recv_sem=mine_r.at[slot],
            device_id={"tm": t, "grp": peer_grp(k)},
            device_id_type=MESH,
        )

    for k in range(1, groups):
        mine_copy(k, g).start()
    for k in range(1, groups):
        mine_copy(k, peer_grp(k)).wait_recv()
    total = mine[0]
    for q in range(1, groups):
        total = total + mine[q]
    right = [total[c : c + 1, :] for c in range(CPAR)]
    white = solve_lower(lower, inverse, right)
    solved = solve_upper(lower, inverse, white)
    for c in range(CPAR):
        ready[c : c + 1, :] = white[c]
        ready[CPAR + c : CPAR + c + 1, :] = solved[c]
    ready[2 * CPAR :, :] = jnp.zeros((16 - 2 * CPAR, width), F32)

    def spread_copy(k, slot):
        return pltpu.make_async_remote_copy(
            src_ref=ready,
            dst_ref=spread.at[slot],
            send_sem=spread_s.at[k],
            recv_sem=spread_r.at[slot],
            device_id={"tm": family + lax.rem(block + k, blocks), "grp": g},
            device_id_type=MESH,
        )

    lax.fori_loop(1, blocks, lambda k, c: (spread_copy(k, block).start(), c)[1], 0)
    spread[block] = ready[...]
    lane = lax.broadcasted_iota(jnp.int32, (1, LANES), 1)
    right_g = []
    for c in range(GPAR):
        row = total[CPAR + c // 2 : CPAR + c // 2 + 1, 0:LANES]
        half = (lane < LANES // 2) if c % 2 == 0 else (lane >= LANES // 2)
        value = jnp.sum(jnp.where(half, row, 0.0), axis=1, keepdims=True)
        right_g.append(jnp.broadcast_to(value, (1, LANES)))
    white_g = solve_lower(lower_g, inverse_g, right_g)
    solved_g = solve_upper(lower_g, inverse_g, white_g)
    for c in range(GPAR):
        glob_ref[c : c + 1, :] = white_g[c]
        glob_ref[GPAR + c : GPAR + c + 1, :] = solved_g[c]
    lax.fori_loop(
        1,
        blocks,
        lambda k, c: (spread_copy(k, lax.rem(block + k, blocks)).wait_recv(), c)[1],
        0,
    )
    out_ref[...] = spread[...]
    lax.fori_loop(1, count, lambda k, c: (whole_copy(k, t).wait_send(), c)[1], 0)
    for k in range(1, groups):
        mine_copy(k, g).wait_send()
    lax.fori_loop(1, blocks, lambda k, c: (spread_copy(k, block).wait_send(), c)[1], 0)


def final_kernel(
    blocks, second_ref, solved_ref, glob_ref, cp_ref, ci_ref, gp_ref, res_ref, step_ref
):
    tiles = second_ref.shape[0]
    units = ci_ref[...]
    high, low = lax.shift_right_logical(units, 7), lax.bitwise_and(units, 127)
    picked = [jnp.zeros((tiles, LANES), F32) for _ in range(CPAR)]
    width = UNITS // blocks
    for row in range(UNITS // LANES):
        block, at = (row * LANES) // width, (row * LANES) % width
        here = high == row
        step_ref[:, row * LANES : (row + 1) * LANES] = solved_ref[block, 0:CPAR, at : at + LANES]
        for c in range(CPAR):
            line = solved_ref[block, CPAR + c : CPAR + c + 1, at : at + LANES]
            table = jnp.broadcast_to(line, (tiles, LANES))
            picked[c] = jnp.where(here, lane_pick(table, low), picked[c])
    out = second_ref[...]
    for c in range(CPAR):
        out = out - cp_ref[c] * picked[c]
    for c in range(GPAR):
        out = out - gp_ref[c] * glob_ref[GPAR + c : GPAR + c + 1, :]
    res_ref[...] = out


def per_device(
    shape, residual, weight, source_part, source_index, source_delta, attitude_part,
    spline_phase, knot_index, calib_part, calib_index, global_part,
):
    count, groups, blocks = shape
    row_count = residual.shape[-1]
    tiles = row_count // TILE
    nodes_dev = tiles * KPT
    width = UNITS // blocks

    def flat(value):
        return value.reshape(tiles, TILE)

    def deep(value):
        return value.reshape(value.shape[0], -1, LANES)

    weights, phase, knots, units = map(flat, (weight, spline_phase, knot_index, calib_index))
    axes, calib, glob = map(deep, (attitude_part, calib_part, global_part))

    def out(*dims):
        return jax.ShapeDtypeStruct(dims, F32)

    dma = pltpu.SemaphoreType.DMA
    first, normals, mats = pl.pallas_call(
        functools.partial(first_kernel, blocks),
        out_shape=(
            out(tiles, LANES), out(NORMAL_ROWS, LANES), out(blocks, NORMAL_ROWS, width),
        ),
        scratch_shapes=[
            pltpu.VMEM((ATT_ROWS * tiles, LANES), F32),
            pltpu.VMEM((UNIT_ROWS * tiles, LANES), F32),
            pltpu.VMEM((ATT_ROWS, LANES), F32),
            pltpu.VMEM((UNIT_ROWS * (UNITS // LOW), LOW), F32),
        ],
        name="first",
    )(
        flat(residual), weights, deep(source_part), flat(source_index), deep(source_delta),
        axes, phase, knots, calib, units, glob,
    )
    x, total = pl.pallas_call(
        functools.partial(attitude_kernel, shape, nodes_dev),
        out_shape=(out(8, LANES), out(NORMAL_ROWS, width)),
        scratch_shapes=[
            pltpu.VMEM((3 * groups, NORMAL_ROWS, LANES), F32),
            pltpu.VMEM((groups, NORMAL_ROWS, width), F32),
            pltpu.VMEM((count, NORMAL_ROWS, width), F32),
            dma((3 * groups,)), dma((3 * groups,)),
            dma((groups,)), dma((groups,)),
            dma((count,)), dma((count,)),
        ],
        in_specs=[pl.BlockSpec(memory_space=pltpu.VMEM)] * 2,
        compiler_params=pltpu.CompilerParams(collective_id=0, has_side_effects=True),
        name="attitude",
    )(normals, mats)
    second, rhs, attitude_step = pl.pallas_call(
        functools.partial(second_kernel, blocks),
        out_shape=(out(tiles, LANES), out(blocks, 8, width), out(3, nodes_dev)),
        scratch_shapes=[
            pltpu.VMEM((8 * tiles, LANES), F32),
            pltpu.VMEM((3 * 8 * (UNITS // LOW), LOW), F32),
        ],
        name="second",
    )(first, x, weights, axes, phase, knots, calib, units, glob)
    solved, global_out = pl.pallas_call(
        functools.partial(solve_kernel, shape),
        out_shape=(out(blocks, 16, width), out(2 * GPAR, LANES)),
        scratch_shapes=[
            pltpu.VMEM((count, 8, width), F32),
            pltpu.VMEM((groups, 8, width), F32),
            pltpu.VMEM((16, width), F32),
            pltpu.VMEM((blocks, 16, width), F32),
            dma((count,)), dma((count,)),
            dma((groups,)), dma((groups,)),
            dma((blocks,)), dma((blocks,)),
        ],
        in_specs=[pl.BlockSpec(memory_space=pltpu.VMEM)] * 2,
        compiler_params=pltpu.CompilerParams(collective_id=1, has_side_effects=True),
        name="solve",
    )(rhs, total)
    final, calib_step = pl.pallas_call(
        functools.partial(final_kernel, blocks),
        out_shape=(out(tiles, LANES), out(CPAR, UNITS)),
        name="final",
    )(second, solved, global_out, calib, units, glob)
    return final.reshape(residual.shape), attitude_step, calib_step, global_out[:GPAR, 0]


def solution(mesh):
    count, groups = mesh.shape["tm"], mesh.shape["grp"]
    blocks = min(count, UNITS // LANES)
    return jax.shard_map(
        functools.partial(per_device, (count, groups, blocks)),
        mesh=mesh,
        in_specs=(
            P("tm", "grp", None),
            P("tm", "grp", None),
            P(None, "tm", "grp", None),
            P("tm", "grp", None),
            P(None, "tm", None),
            P(None, "tm", "grp", None),
            P("tm", "grp", None),
            P("tm", "grp", None),
            P(None, "tm", "grp", None),
            P("tm", "grp", None),
            P(None, "tm", "grp", None),
        ),
        out_specs=(P("tm", "grp", None), P(None, "tm"), P(), P()),
        check_vma=False,
    )
```

```python
import functools

import jax
import jax.numpy as jnp
from jax import lax
from jax.experimental import pallas as pl
from jax.experimental.pallas import tpu as pltpu
from jax.sharding import PartitionSpec as P

TILE = 128
KPT = 4
UNITS = 2048
CPAR = 6
GPAR = 4
ATT_SWEEPS = 4

OMEGA = 0.6
RIDGE = 1.0
LANES = 128
LOW = 256
HALO = 3 * ATT_SWEEPS
MESH = pl.DeviceIdType.MESH
F32 = jnp.float32
BF16 = jnp.bfloat16

ATT_ROWS = 72
UNIT_ROWS = 24
NORMAL_ROWS = 32


def pairs_of(extent):
    return [(a, b) for a in range(extent) for b in range(a, extent)]


def lane_pick(table, index):
    return lax.gather(
        table,
        index[..., None],
        lax.GatherDimensionNumbers(
            offset_dims=(),
            collapsed_slice_dims=(1,),
            start_index_map=(1,),
            operand_batching_dims=(0,),
            start_indices_batching_dims=(0,),
        ),
        (1, 1),
        mode=lax.GatherScatterMode.PROMISE_IN_BOUNDS,
    )


def spline_basis(phase):
    inverse = 1.0 - phase
    square = phase * phase
    cubed = square * phase
    return [
        inverse * inverse * inverse / 6.0,
        (3.0 * cubed - 6.0 * square + 4.0) / 6.0,
        (-3.0 * cubed + 3.0 * square + 3.0 * phase + 1.0) / 6.0,
        cubed / 6.0,
    ]


def cholesky_lists(matrix, extent):
    lower = [[None] * extent for _ in range(extent)]
    inverse = [None] * extent
    for column in range(extent):
        pivot = matrix[column][column]
        for k in range(column):
            pivot = pivot - lower[column][k] * lower[column][k]
        root = jnp.sqrt(pivot)
        lower[column][column] = root
        inverse[column] = 1.0 / root
        for row in range(column + 1, extent):
            entry = matrix[row][column]
            for k in range(column):
                entry = entry - lower[row][k] * lower[column][k]
            lower[row][column] = entry * inverse[column]
    return lower, inverse


def solve_lower(lower, inverse, vector):
    result = []
    for row in range(len(vector)):
        running = vector[row]
        for k in range(row):
            running = running - lower[row][k] * result[k]
        result.append(running * inverse[row])
    return result


def solve_upper(lower, inverse, vector):
    extent = len(vector)
    result = [None] * extent
    for row in reversed(range(extent)):
        running = vector[row]
        for k in range(row + 1, extent):
            running = running - lower[k][row] * result[k]
        result[row] = running * inverse[row]
    return result


def symmetric(upper, extent):
    matrix = [[None] * extent for _ in range(extent)]
    for position, (a, b) in enumerate(pairs_of(extent)):
        value = upper[position] + (RIDGE if a == b else 0.0)
        matrix[a][b] = value
        matrix[b][a] = value
    return matrix


def split_three(value):
    first = value.astype(BF16).astype(F32)
    rest = value - first
    second = rest.astype(BF16).astype(F32)
    third = (rest - second).astype(BF16).astype(F32)
    return [first, second, third]


def dot_nt(left, right):
    return lax.dot_general(
        left, right, (((1,), (1,)), ((), ())), preferred_element_type=F32
    )


def two_tiles(ref, tile, rows, tiles):
    return jnp.concatenate(
        [ref[pl.ds(tile, rows, stride=tiles), :], ref[pl.ds(tile + 1, rows, stride=tiles), :]],
        axis=1,
    )


def two_rows(ref, tile):
    return jnp.concatenate([ref[pl.ds(tile, 1), :], ref[pl.ds(tile + 1, 1), :]], axis=1)


def one_hot(row, extent):
    spots = lax.broadcasted_iota(jnp.int32, (extent, row.shape[1]), 0)
    return jnp.where(spots == row, 1.0, 0.0).astype(BF16)


def by_high(part, high):
    return jnp.concatenate(
        [jnp.where(high == h, part, 0.0) for h in range(UNITS // LOW)], axis=0
    )


def block_pieces(blocks):
    width = UNITS // blocks
    for piece in range(UNITS // LANES):
        unit = piece * LANES
        yield unit // width, unit % width, unit // LOW, unit % LOW


def step_kernel(
    shape, nodes_dev, res_ref, w_ref, sp_ref, si_ref, sd_ref, ap_ref, ph_ref, kn_ref, cp_ref,
    ci_ref, gp_ref, second_ref, step_ref, out_ref, glob_ref,
    att, cal, rcal, acc_att, acc_cal, acc_rhs, normal_ref, mats_ref, rhs_ref,
    near, mine, whole, rwhole, rmine, ready, spread,
    near_s, near_r, mine_s, mine_r, whole_s, whole_r,
    rwhole_s, rwhole_r, rmine_s, rmine_r, spread_s, spread_r,
):
    count, groups, blocks = shape
    t, g = lax.axis_index("tm"), lax.axis_index("grp")
    has_before, has_after = t > 0, t < count - 1

    def peer_tm(k):
        return lax.rem(t + k, count)

    def peer_grp(k):
        return lax.rem(g + k, groups)

    barrier = pltpu.get_barrier_semaphore()

    def greet(where):
        pl.semaphore_signal(barrier, inc=1, device_id=where, device_id_type=MESH)

    lax.fori_loop(1, count, lambda k, c: (greet({"tm": peer_tm(k), "grp": g}), c)[1], 0)
    for k in range(1, groups):
        greet({"tm": t, "grp": peer_grp(k)})
        greet({"tm": peer_tm(1), "grp": peer_grp(k)})
        greet({"tm": peer_tm(count - 1), "grp": peer_grp(k)})
    tiles = res_ref.shape[0]
    weights = w_ref[...]
    sources = si_ref[...]
    high, low = lax.shift_right_logical(sources, 7), lax.bitwise_and(sources, 127)
    picked = [jnp.zeros((tiles, LANES), F32) for _ in range(5)]
    for row in range(sd_ref.shape[1]):
        here = high == row
        for c in range(5):
            table = jnp.broadcast_to(sd_ref[c, row : row + 1, :], (tiles, LANES))
            picked[c] = jnp.where(here, lane_pick(table, low), picked[c])
    total = sp_ref[0] * picked[0]
    for c in range(1, 5):
        total = total + sp_ref[c] * picked[c]
    first = res_ref[...] - total
    basis = spline_basis(ph_ref[...])
    axes = [ap_ref[c] for c in range(3)]
    products = [weights * axes[a] * axes[b] for a, b in pairs_of(3)]
    rights = [weights * axes[a] * first for a in range(3)]
    place = 0
    for i in range(4):
        for d in range(4 - i):
            both = basis[i] * basis[i + d]
            for product in products:
                att[place * tiles : (place + 1) * tiles, :] = both * product
                place += 1
    for i in range(4):
        for right in rights:
            att[place * tiles : (place + 1) * tiles, :] = basis[i] * right
            place += 1
    acc_att[...] = jnp.zeros_like(acc_att)
    base = lax.axis_index("tm") * (tiles * KPT)

    def bin_nodes(no, carry):
        tile = no * 2
        knots = two_rows(kn_ref, tile) - base
        nodes = one_hot(knots, LANES)
        part = acc_att[...]
        for piece in split_three(two_tiles(att, tile, ATT_ROWS, tiles)):
            part = part + dot_nt(piece.astype(BF16), nodes)
        acc_att[...] = part
        return carry

    lax.fori_loop(0, tiles // 2, bin_nodes, 0, unroll=2)
    band = [None] * 5
    place = 0
    for i in range(4):
        for d in list(range(4 - i)):
            rows = acc_att[place : place + 6, :]
            rows = pltpu.roll(rows, i, 1) if i else rows
            band[d] = rows if band[d] is None else band[d] + rows
            place += 6
    for i in range(4):
        rows = acc_att[place : place + 3, :]
        rows = pltpu.roll(rows, i, 1) if i else rows
        band[4] = rows if band[4] is None else band[4] + rows
        place += 3
    for d in range(4):
        normal_ref[d * 6 : (d + 1) * 6, :] = band[d]
    normal_ref[24:27, :] = band[4]
    normal_ref[27:, :] = jnp.zeros((NORMAL_ROWS - 27, LANES), F32)
    pl.semaphore_wait(barrier, count - 1 + 3 * (groups - 1))

    def near_copy(offset, k):
        slot = (1 - offset) * groups + g
        return pltpu.make_async_remote_copy(
            src_ref=normal_ref,
            dst_ref=near.at[slot],
            send_sem=near_s.at[(offset + 1) * groups + k],
            recv_sem=near_r.at[slot],
            device_id={"tm": t + offset, "grp": peer_grp(k)},
            device_id_type=MESH,
        )

    def near_arrival(offset, k):
        slot = (offset + 1) * groups + peer_grp(k)
        return pltpu.make_async_remote_copy(
            src_ref=normal_ref,
            dst_ref=near.at[slot],
            send_sem=near_s.at[(offset + 1) * groups + k],
            recv_sem=near_r.at[slot],
            device_id={"tm": t + offset, "grp": peer_grp(k)},
            device_id_type=MESH,
        )

    def each_near(do):
        for k in range(1, groups):
            do(0, k)

        @pl.when(has_before)
        def _():
            for k in range(groups):
                do(-1, k)

        @pl.when(has_after)
        def _():
            for k in range(groups):
                do(1, k)

    each_near(lambda offset, k: near_copy(offset, k).start())

    place = 0
    for a, b in pairs_of(CPAR):
        cal[place * tiles : (place + 1) * tiles, :] = weights * cp_ref[a] * cp_ref[b]
        place += 1
    cal[place * tiles :, :] = jnp.zeros(((UNIT_ROWS - place) * tiles, LANES), F32)
    global_rows = [
        jnp.sum(weights * gp_ref[a] * gp_ref[b], axis=0, keepdims=True)
        for a, b in pairs_of(GPAR)
    ]
    acc_cal[...] = jnp.zeros_like(acc_cal)

    def bin_units(no, carry):
        tile = no * 2
        units = two_rows(ci_ref, tile)
        upper, lower = lax.shift_right_logical(units, 8), lax.bitwise_and(units, 255)
        spots = one_hot(lower, LOW)
        part = acc_cal[...]
        for piece in split_three(two_tiles(cal, tile, UNIT_ROWS, tiles)):
            part = part + dot_nt(by_high(piece, upper).astype(BF16), spots)
        acc_cal[...] = part
        return carry

    lax.fori_loop(0, tiles // 2, bin_units, 0, unroll=2)
    mats_ref[...] = jnp.zeros_like(mats_ref)
    for block, at, h, start in block_pieces(blocks):
        mats_ref[block, 0:21, at : at + LANES] = acc_cal[
            h * UNIT_ROWS : h * UNIT_ROWS + 21, start : start + LANES
        ]
        if at == 0:
            for no, row in enumerate(global_rows):
                mats_ref[block, 21 + no : 22 + no, 0:LANES] = row

    def whole_copy(k):
        p = peer_tm(k)
        return pltpu.make_async_remote_copy(
            src_ref=mats_ref.at[lax.rem(p, blocks)],
            dst_ref=whole.at[t],
            send_sem=whole_s.at[k],
            recv_sem=whole_r.at[t],
            device_id={"tm": p, "grp": g},
            device_id_type=MESH,
        )

    def whole_arrival(k):
        p = peer_tm(k)
        return pltpu.make_async_remote_copy(
            src_ref=mats_ref.at[lax.rem(p, blocks)],
            dst_ref=whole.at[p],
            send_sem=whole_s.at[k],
            recv_sem=whole_r.at[p],
            device_id={"tm": p, "grp": g},
            device_id_type=MESH,
        )

    lax.fori_loop(1, count, lambda k, c: (whole_copy(k).start(), c)[1], 0)
    whole[t] = mats_ref[lax.rem(t, blocks)]
    near[groups + g] = normal_ref[...]

    @pl.when(jnp.logical_not(has_before))
    def _():
        near[0:groups] = jnp.zeros((groups, NORMAL_ROWS, LANES), F32)

    @pl.when(jnp.logical_not(has_after))
    def _():
        near[2 * groups :] = jnp.zeros((groups, NORMAL_ROWS, LANES), F32)

    each_near(lambda offset, k: near_arrival(offset, k).wait_recv())
    sums = []
    for s in range(3):
        part = near[s * groups]
        for q in range(1, groups):
            part = part + near[s * groups + q]
        sums.append(part)
    lane = lax.broadcasted_iota(jnp.int32, (NORMAL_ROWS, LANES), 1)
    before = pltpu.roll(sums[0], (HALO - nodes_dev) % LANES, 1)
    own = pltpu.roll(sums[1], HALO, 1)
    after = pltpu.roll(sums[2], (HALO + nodes_dev) % LANES, 1)
    end = nodes_dev + HALO
    normals = (
        own
        + jnp.where((lane >= 3) & (lane < HALO + 3), before, 0.0)
        + jnp.where((lane >= end) & (lane < end + HALO), after, 0.0)
    )
    spot = lax.broadcasted_iota(jnp.int32, (1, LANES), 1)
    exists = (spot >= jnp.where(has_before, 0, HALO)) & (
        spot < jnp.where(has_after, LANES, end)
    )
    normals = jnp.where(exists, normals, 0.0)
    index = {}
    for position, (a, b) in enumerate(pairs_of(3)):
        index[a, b] = index[b, a] = position
    band = [[normals[d * 6 + p : d * 6 + p + 1, :] for p in range(6)] for d in range(4)]
    right = [normals[24 + c : 25 + c, :] for c in range(3)]
    lower, inverse = cholesky_lists(symmetric(band[0], 3), 3)

    def precondition(vector):
        return solve_upper(lower, inverse, solve_lower(lower, inverse, vector))

    x = [OMEGA * value for value in precondition(right)]
    for _ in range(1, ATT_SWEEPS):
        out = [right[c] - x[c] for c in range(3)]
        for d in range(4):
            ahead = [pltpu.roll(x[c], LANES - d, 1) for c in range(3)] if d else x
            for a in range(3):
                for b in range(3):
                    out[a] = out[a] - band[d][index[a, b]] * ahead[b]
        for d in range(1, 4):
            for a in range(3):
                term = band[d][index[a, 0]] * x[0]
                for b in range(1, 3):
                    term = term + band[d][index[a, b]] * x[b]
                out[a] = out[a] - pltpu.roll(term, d, 1)
        change = precondition(out)
        x = [jnp.where(exists, x[c] + OMEGA * change[c], 0.0) for c in range(3)]
    for c in range(3):
        scaled = lower[c][c] * x[c]
        for k in range(c + 1, 3):
            scaled = scaled + lower[k][c] * x[k]
        moved = pltpu.roll(scaled, LANES - HALO, 1)
        step_ref[c : c + 1, :] = moved[:, 0:nodes_dev]


    local = kn_ref[...] - base + HALO
    tables = [jnp.broadcast_to(x[c], (tiles, LANES)) for c in range(3)]
    second = first
    for i in range(4):
        moved = ap_ref[0] * lane_pick(tables[0], local + i)
        for c in range(1, 3):
            moved = moved + ap_ref[c] * lane_pick(tables[c], local + i)
        second = second - basis[i] * moved
    second_ref[...] = second
    weighted = weights * second
    for a in range(CPAR):
        rcal[a * tiles : (a + 1) * tiles, :] = weighted * cp_ref[a]
    rcal[CPAR * tiles :, :] = jnp.zeros(((8 - CPAR) * tiles, LANES), F32)
    sums = [jnp.sum(weighted * gp_ref[a], axis=0, keepdims=True) for a in range(GPAR)]
    acc_rhs[...] = jnp.zeros_like(acc_rhs)

    def bin_rhs(no, carry):
        tile = no * 2
        units = two_rows(ci_ref, tile)
        upper, lower = lax.shift_right_logical(units, 8), lax.bitwise_and(units, 255)
        pieces = [by_high(p, upper) for p in split_three(two_tiles(rcal, tile, 8, tiles))]
        lhs = jnp.concatenate(pieces, axis=0).astype(BF16)
        acc_rhs[...] = acc_rhs[...] + dot_nt(lhs, one_hot(lower, LOW))
        return carry

    lax.fori_loop(0, tiles // 2, bin_rhs, 0, unroll=2)
    rows = 8 * (UNITS // LOW)
    total = acc_rhs[0:rows, :] + acc_rhs[rows : 2 * rows, :] + acc_rhs[2 * rows : 3 * rows, :]
    lane = lax.broadcasted_iota(jnp.int32, (1, LANES), 1)
    folded = [row + pltpu.roll(row, LANES // 2, 1) for row in sums]
    packed = [jnp.where(lane < LANES // 2, folded[2 * k], folded[2 * k + 1]) for k in range(2)]
    if rhs_ref.shape[2] > LANES:
        rhs_ref[...] = jnp.zeros_like(rhs_ref)
    for block, at, h, start in block_pieces(blocks):
        rhs_ref[block, 0:CPAR, at : at + LANES] = total[
            h * 8 : h * 8 + CPAR, start : start + LANES
        ]
        if at == 0:
            for k in range(2):
                rhs_ref[block, CPAR + k : CPAR + k + 1, 0:LANES] = packed[k]

    width = rhs_ref.shape[2]
    block = lax.rem(t, blocks)
    family = t - block

    def rwhole_copy(k, slot):
        p = peer_tm(k)
        return pltpu.make_async_remote_copy(
            src_ref=rhs_ref.at[lax.rem(p, blocks)],
            dst_ref=rwhole.at[slot],
            send_sem=rwhole_s.at[k],
            recv_sem=rwhole_r.at[slot],
            device_id={"tm": p, "grp": g},
            device_id_type=MESH,
        )

    lax.fori_loop(1, count, lambda k, c: (rwhole_copy(k, t).start(), c)[1], 0)
    rwhole[t] = rhs_ref[block]
    lax.fori_loop(1, count, lambda k, c: (whole_arrival(k).wait_recv(), c)[1], 0)
    mine[g] = lax.fori_loop(1, count, lambda k, c: c + whole[k], whole[0])

    def mine_copy(k):
        return pltpu.make_async_remote_copy(
            src_ref=mine.at[g],
            dst_ref=mine.at[g],
            send_sem=mine_s.at[k],
            recv_sem=mine_r.at[g],
            device_id={"tm": t, "grp": peer_grp(k)},
            device_id_type=MESH,
        )

    def mine_arrival(k):
        q = peer_grp(k)
        return pltpu.make_async_remote_copy(
            src_ref=mine.at[q],
            dst_ref=mine.at[q],
            send_sem=mine_s.at[k],
            recv_sem=mine_r.at[q],
            device_id={"tm": t, "grp": q},
            device_id_type=MESH,
        )

    for k in range(1, groups):
        mine_copy(k).start()
    for k in range(1, groups):
        mine_arrival(k).wait_recv()
    total = mine[0]
    for q in range(1, groups):
        total = total + mine[q]
    unit_total = total
    matrix = [unit_total[p : p + 1, :] for p in range(21)]
    lower, inverse = cholesky_lists(symmetric(matrix, CPAR), CPAR)
    upper_g = [
        jnp.broadcast_to(
            jnp.sum(unit_total[21 + p : 22 + p, 0:LANES], axis=1, keepdims=True), (1, LANES)
        )
        for p in range(10)
    ]
    lower_g, inverse_g = cholesky_lists(symmetric(upper_g, GPAR), GPAR)
    lax.fori_loop(1, count, lambda k, c: (rwhole_copy(k, peer_tm(k)).wait_recv(), c)[1], 0)
    rmine[g] = lax.fori_loop(1, count, lambda k, c: c + rwhole[k], rwhole[0])

    def rmine_copy(k, slot):
        return pltpu.make_async_remote_copy(
            src_ref=rmine.at[slot],
            dst_ref=rmine.at[slot],
            send_sem=rmine_s.at[k],
            recv_sem=rmine_r.at[slot],
            device_id={"tm": t, "grp": peer_grp(k)},
            device_id_type=MESH,
        )

    for k in range(1, groups):
        rmine_copy(k, g).start()
    for k in range(1, groups):
        rmine_copy(k, peer_grp(k)).wait_recv()
    total = rmine[0]
    for q in range(1, groups):
        total = total + rmine[q]
    right = [total[c : c + 1, :] for c in range(CPAR)]
    white = solve_lower(lower, inverse, right)
    solved = solve_upper(lower, inverse, white)
    for c in range(CPAR):
        ready[c : c + 1, :] = white[c]
        ready[CPAR + c : CPAR + c + 1, :] = solved[c]
    ready[2 * CPAR :, :] = jnp.zeros((16 - 2 * CPAR, width), F32)

    def spread_copy(k, slot):
        return pltpu.make_async_remote_copy(
            src_ref=ready,
            dst_ref=spread.at[slot],
            send_sem=spread_s.at[k],
            recv_sem=spread_r.at[slot],
            device_id={"tm": family + lax.rem(block + k, blocks), "grp": g},
            device_id_type=MESH,
        )

    lax.fori_loop(1, blocks, lambda k, c: (spread_copy(k, block).start(), c)[1], 0)
    spread[block] = ready[...]
    lane = lax.broadcasted_iota(jnp.int32, (1, LANES), 1)
    right_g = []
    for c in range(GPAR):
        row = total[CPAR + c // 2 : CPAR + c // 2 + 1, 0:LANES]
        half = (lane < LANES // 2) if c % 2 == 0 else (lane >= LANES // 2)
        value = jnp.sum(jnp.where(half, row, 0.0), axis=1, keepdims=True)
        right_g.append(jnp.broadcast_to(value, (1, LANES)))
    white_g = solve_lower(lower_g, inverse_g, right_g)
    solved_g = solve_upper(lower_g, inverse_g, white_g)
    for c in range(GPAR):
        glob_ref[c : c + 1, :] = white_g[c]
        glob_ref[GPAR + c : GPAR + c + 1, :] = solved_g[c]
    lax.fori_loop(
        1,
        blocks,
        lambda k, c: (spread_copy(k, lax.rem(block + k, blocks)).wait_recv(), c)[1],
        0,
    )
    out_ref[...] = spread[...]
    lax.fori_loop(1, count, lambda k, c: (rwhole_copy(k, t).wait_send(), c)[1], 0)
    for k in range(1, groups):
        rmine_copy(k, g).wait_send()
    lax.fori_loop(1, blocks, lambda k, c: (spread_copy(k, block).wait_send(), c)[1], 0)
    for k in range(1, groups):
        mine_copy(k).wait_send()
    each_near(lambda offset, k: near_copy(offset, k).wait_send())
    lax.fori_loop(1, count, lambda k, c: (whole_copy(k).wait_send(), c)[1], 0)


def final_kernel(
    blocks, second_ref, solved_ref, glob_ref, cp_ref, ci_ref, gp_ref, res_ref, step_ref
):
    tiles = second_ref.shape[0]
    units = ci_ref[...]
    high, low = lax.shift_right_logical(units, 7), lax.bitwise_and(units, 127)
    picked = [jnp.zeros((tiles, LANES), F32) for _ in range(CPAR)]
    width = UNITS // blocks
    for row in range(UNITS // LANES):
        block, at = (row * LANES) // width, (row * LANES) % width
        here = high == row
        step_ref[:, row * LANES : (row + 1) * LANES] = solved_ref[block, 0:CPAR, at : at + LANES]
        for c in range(CPAR):
            line = solved_ref[block, CPAR + c : CPAR + c + 1, at : at + LANES]
            table = jnp.broadcast_to(line, (tiles, LANES))
            picked[c] = jnp.where(here, lane_pick(table, low), picked[c])
    out = second_ref[...]
    for c in range(CPAR):
        out = out - cp_ref[c] * picked[c]
    for c in range(GPAR):
        out = out - gp_ref[c] * glob_ref[GPAR + c : GPAR + c + 1, :]
    res_ref[...] = out


def per_device(
    shape, residual, weight, source_part, source_index, source_delta, attitude_part,
    spline_phase, knot_index, calib_part, calib_index, global_part,
):
    count, groups, blocks = shape
    row_count = residual.shape[-1]
    tiles = row_count // TILE
    nodes_dev = tiles * KPT
    width = UNITS // blocks

    def flat(value):
        return value.reshape(tiles, TILE)

    def deep(value):
        return value.reshape(value.shape[0], -1, LANES)

    weights, phase, knots, units = map(flat, (weight, spline_phase, knot_index, calib_index))
    axes, calib, glob = map(deep, (attitude_part, calib_part, global_part))

    def out(*dims):
        return jax.ShapeDtypeStruct(dims, F32)

    dma = pltpu.SemaphoreType.DMA
    second, attitude_step, solved, global_out = pl.pallas_call(
        functools.partial(step_kernel, shape, nodes_dev),
        out_shape=(
            out(tiles, LANES), out(3, nodes_dev), out(blocks, 16, width), out(2 * GPAR, LANES),
        ),
        scratch_shapes=[
            pltpu.VMEM((ATT_ROWS * tiles, LANES), F32),
            pltpu.VMEM((UNIT_ROWS * tiles, LANES), F32),
            pltpu.VMEM((8 * tiles, LANES), F32),
            pltpu.VMEM((ATT_ROWS, LANES), F32),
            pltpu.VMEM((UNIT_ROWS * (UNITS // LOW), LOW), F32),
            pltpu.VMEM((3 * 8 * (UNITS // LOW), LOW), F32),
            pltpu.VMEM((NORMAL_ROWS, LANES), F32),
            pltpu.VMEM((blocks, NORMAL_ROWS, width), F32),
            pltpu.VMEM((blocks, 8, width), F32),
            pltpu.VMEM((3 * groups, NORMAL_ROWS, LANES), F32),
            pltpu.VMEM((groups, NORMAL_ROWS, width), F32),
            pltpu.VMEM((count, NORMAL_ROWS, width), F32),
            pltpu.VMEM((count, 8, width), F32),
            pltpu.VMEM((groups, 8, width), F32),
            pltpu.VMEM((16, width), F32),
            pltpu.VMEM((blocks, 16, width), F32),
            dma((3 * groups,)), dma((3 * groups,)),
            dma((groups,)), dma((groups,)),
            dma((count,)), dma((count,)),
            dma((count,)), dma((count,)),
            dma((groups,)), dma((groups,)),
            dma((blocks,)), dma((blocks,)),
        ],
        in_specs=[pl.BlockSpec(memory_space=pltpu.VMEM)] * 11,
        compiler_params=pltpu.CompilerParams(collective_id=0, has_side_effects=True),
        name="step",
    )(
        flat(residual), weights, deep(source_part), flat(source_index), deep(source_delta),
        axes, phase, knots, calib, units, glob,
    )
    final, calib_step = pl.pallas_call(
        functools.partial(final_kernel, blocks),
        out_shape=(out(tiles, LANES), out(CPAR, UNITS)),
        name="final",
    )(second, solved, global_out, calib, units, glob)
    return final.reshape(residual.shape), attitude_step, calib_step, global_out[:GPAR, 0]


def solution(mesh):
    count, groups = mesh.shape["tm"], mesh.shape["grp"]
    blocks = min(count, UNITS // LANES)
    return jax.shard_map(
        functools.partial(per_device, (count, groups, blocks)),
        mesh=mesh,
        in_specs=(
            P("tm", "grp", None),
            P("tm", "grp", None),
            P(None, "tm", "grp", None),
            P("tm", "grp", None),
            P(None, "tm", None),
            P(None, "tm", "grp", None),
            P("tm", "grp", None),
            P("tm", "grp", None),
            P(None, "tm", "grp", None),
            P("tm", "grp", None),
            P(None, "tm", "grp", None),
        ),
        out_specs=(P("tm", "grp", None), P(None, "tm"), P(), P()),
        check_vma=False,
    )
```

```python
import functools

import jax
import jax.numpy as jnp
from jax import lax
from jax.experimental import pallas as pl
from jax.experimental.pallas import tpu as pltpu
from jax.sharding import PartitionSpec as P

TILE = 128
KPT = 4
UNITS = 2048
CPAR = 6
GPAR = 4
ATT_SWEEPS = 4

OMEGA = 0.6
RIDGE = 1.0
LANES = 128
LOW = 256
HALO = 3 * ATT_SWEEPS
MESH = pl.DeviceIdType.MESH
F32 = jnp.float32
BF16 = jnp.bfloat16

ATT_ROWS = 72
UNIT_ROWS = 24
NORMAL_ROWS = 32


def pairs_of(extent):
    return [(a, b) for a in range(extent) for b in range(a, extent)]


def lane_pick(table, index):
    return lax.gather(
        table,
        index[..., None],
        lax.GatherDimensionNumbers(
            offset_dims=(),
            collapsed_slice_dims=(1,),
            start_index_map=(1,),
            operand_batching_dims=(0,),
            start_indices_batching_dims=(0,),
        ),
        (1, 1),
        mode=lax.GatherScatterMode.PROMISE_IN_BOUNDS,
    )


def spline_basis(phase):
    inverse = 1.0 - phase
    square = phase * phase
    cubed = square * phase
    return [
        inverse * inverse * inverse / 6.0,
        (3.0 * cubed - 6.0 * square + 4.0) / 6.0,
        (-3.0 * cubed + 3.0 * square + 3.0 * phase + 1.0) / 6.0,
        cubed / 6.0,
    ]


def cholesky_lists(matrix, extent):
    lower = [[None] * extent for _ in range(extent)]
    inverse = [None] * extent
    for column in range(extent):
        pivot = matrix[column][column]
        for k in range(column):
            pivot = pivot - lower[column][k] * lower[column][k]
        root = jnp.sqrt(pivot)
        lower[column][column] = root
        inverse[column] = 1.0 / root
        for row in range(column + 1, extent):
            entry = matrix[row][column]
            for k in range(column):
                entry = entry - lower[row][k] * lower[column][k]
            lower[row][column] = entry * inverse[column]
    return lower, inverse


def solve_lower(lower, inverse, vector):
    result = []
    for row in range(len(vector)):
        running = vector[row]
        for k in range(row):
            running = running - lower[row][k] * result[k]
        result.append(running * inverse[row])
    return result


def solve_upper(lower, inverse, vector):
    extent = len(vector)
    result = [None] * extent
    for row in reversed(range(extent)):
        running = vector[row]
        for k in range(row + 1, extent):
            running = running - lower[k][row] * result[k]
        result[row] = running * inverse[row]
    return result


def symmetric(upper, extent):
    matrix = [[None] * extent for _ in range(extent)]
    for position, (a, b) in enumerate(pairs_of(extent)):
        value = upper[position] + (RIDGE if a == b else 0.0)
        matrix[a][b] = value
        matrix[b][a] = value
    return matrix


def split_three(value):
    first = value.astype(BF16).astype(F32)
    rest = value - first
    second = rest.astype(BF16).astype(F32)
    third = (rest - second).astype(BF16).astype(F32)
    return [first, second, third]


def dot_nt(left, right):
    return lax.dot_general(
        left, right, (((1,), (1,)), ((), ())), preferred_element_type=F32
    )


def two_tiles(ref, tile, rows, tiles):
    return jnp.concatenate(
        [ref[pl.ds(tile, rows, stride=tiles), :], ref[pl.ds(tile + 1, rows, stride=tiles), :]],
        axis=1,
    )


def two_rows(ref, tile):
    return jnp.concatenate([ref[pl.ds(tile, 1), :], ref[pl.ds(tile + 1, 1), :]], axis=1)


def one_hot(row, extent):
    spots = lax.broadcasted_iota(jnp.int32, (extent, row.shape[1]), 0)
    return jnp.where(spots == row, 1.0, 0.0).astype(BF16)


def by_high(part, high):
    return jnp.concatenate(
        [jnp.where(high == h, part, 0.0) for h in range(UNITS // LOW)], axis=0
    )


def block_pieces(blocks):
    width = UNITS // blocks
    for piece in range(UNITS // LANES):
        unit = piece * LANES
        yield unit // width, unit % width, unit // LOW, unit % LOW


def step_kernel(
    shape, nodes_dev, res_ref, w_ref, sp_ref, si_ref, sd_ref, ap_ref, ph_ref, kn_ref, cp_ref,
    ci_ref, gp_ref, second_ref, step_ref, out_ref, glob_ref,
    att, cal, rcal, acc_att, acc_cal, acc_rhs, normal_ref, mats_ref, rhs_ref,
    near, mine, whole, rwhole, rmine, ready, spread,
    near_s, near_r, mine_s, mine_r, whole_s, whole_r,
    rwhole_s, rwhole_r, rmine_s, rmine_r, spread_s, spread_r,
):
    count, groups, blocks = shape
    t, g = lax.axis_index("tm"), lax.axis_index("grp")
    has_before, has_after = t > 0, t < count - 1

    def peer_tm(k):
        return lax.rem(t + k, count)

    def peer_grp(k):
        return lax.rem(g + k, groups)

    barrier = pltpu.get_barrier_semaphore()

    def greet(where):
        pl.semaphore_signal(barrier, inc=1, device_id=where, device_id_type=MESH)

    lax.fori_loop(1, count, lambda k, c: (greet({"tm": peer_tm(k), "grp": g}), c)[1], 0)
    for k in range(1, groups):
        greet({"tm": t, "grp": peer_grp(k)})
        greet({"tm": peer_tm(1), "grp": peer_grp(k)})
        greet({"tm": peer_tm(count - 1), "grp": peer_grp(k)})
    tiles = res_ref.shape[0]
    weights = w_ref[...]
    sources = si_ref[...]
    high, low = lax.shift_right_logical(sources, 7), lax.bitwise_and(sources, 127)
    picked = [jnp.zeros((tiles, LANES), F32) for _ in range(5)]
    for row in range(sd_ref.shape[1]):
        here = high == row
        for c in range(5):
            table = jnp.broadcast_to(sd_ref[c, row : row + 1, :], (tiles, LANES))
            picked[c] = jnp.where(here, lane_pick(table, low), picked[c])
    total = sp_ref[0] * picked[0]
    for c in range(1, 5):
        total = total + sp_ref[c] * picked[c]
    first = res_ref[...] - total
    basis = spline_basis(ph_ref[...])
    axes = [ap_ref[c] for c in range(3)]
    products = [weights * axes[a] * axes[b] for a, b in pairs_of(3)]
    rights = [weights * axes[a] * first for a in range(3)]
    place = 0
    for i in range(4):
        for d in range(4 - i):
            both = basis[i] * basis[i + d]
            for product in products:
                att[place * tiles : (place + 1) * tiles, :] = both * product
                place += 1
    for i in range(4):
        for right in rights:
            att[place * tiles : (place + 1) * tiles, :] = basis[i] * right
            place += 1
    acc_att[...] = jnp.zeros_like(acc_att)
    base = lax.axis_index("tm") * (tiles * KPT)

    def bin_nodes(no, carry):
        tile = no * 2
        knots = two_rows(kn_ref, tile) - base
        nodes = one_hot(knots, LANES)
        part = acc_att[...]
        for piece in split_three(two_tiles(att, tile, ATT_ROWS, tiles)):
            part = part + dot_nt(piece.astype(BF16), nodes)
        acc_att[...] = part
        return carry

    lax.fori_loop(0, tiles // 2, bin_nodes, 0, unroll=6)
    band = [None] * 5
    place = 0
    for i in range(4):
        for d in list(range(4 - i)):
            rows = acc_att[place : place + 6, :]
            rows = pltpu.roll(rows, i, 1) if i else rows
            band[d] = rows if band[d] is None else band[d] + rows
            place += 6
    for i in range(4):
        rows = acc_att[place : place + 3, :]
        rows = pltpu.roll(rows, i, 1) if i else rows
        band[4] = rows if band[4] is None else band[4] + rows
        place += 3
    for d in range(4):
        normal_ref[d * 6 : (d + 1) * 6, :] = band[d]
    normal_ref[24:27, :] = band[4]
    normal_ref[27:, :] = jnp.zeros((NORMAL_ROWS - 27, LANES), F32)
    pl.semaphore_wait(barrier, count - 1 + 3 * (groups - 1))

    def near_copy(offset, k):
        slot = (1 - offset) * groups + g
        return pltpu.make_async_remote_copy(
            src_ref=normal_ref,
            dst_ref=near.at[slot],
            send_sem=near_s.at[(offset + 1) * groups + k],
            recv_sem=near_r.at[slot],
            device_id={"tm": t + offset, "grp": peer_grp(k)},
            device_id_type=MESH,
        )

    def near_arrival(offset, k):
        slot = (offset + 1) * groups + peer_grp(k)
        return pltpu.make_async_remote_copy(
            src_ref=normal_ref,
            dst_ref=near.at[slot],
            send_sem=near_s.at[(offset + 1) * groups + k],
            recv_sem=near_r.at[slot],
            device_id={"tm": t + offset, "grp": peer_grp(k)},
            device_id_type=MESH,
        )

    def each_near(do):
        for k in range(1, groups):
            do(0, k)

        @pl.when(has_before)
        def _():
            for k in range(groups):
                do(-1, k)

        @pl.when(has_after)
        def _():
            for k in range(groups):
                do(1, k)

    each_near(lambda offset, k: near_copy(offset, k).start())

    place = 0
    for a, b in pairs_of(CPAR):
        cal[place * tiles : (place + 1) * tiles, :] = weights * cp_ref[a] * cp_ref[b]
        place += 1
    cal[place * tiles :, :] = jnp.zeros(((UNIT_ROWS - place) * tiles, LANES), F32)
    global_rows = [
        jnp.sum(weights * gp_ref[a] * gp_ref[b], axis=0, keepdims=True)
        for a, b in pairs_of(GPAR)
    ]
    acc_cal[...] = jnp.zeros_like(acc_cal)

    def bin_units(no, carry):
        tile = no * 2
        units = two_rows(ci_ref, tile)
        upper, lower = lax.shift_right_logical(units, 8), lax.bitwise_and(units, 255)
        spots = one_hot(lower, LOW)
        part = acc_cal[...]
        for piece in split_three(two_tiles(cal, tile, UNIT_ROWS, tiles)):
            part = part + dot_nt(by_high(piece, upper).astype(BF16), spots)
        acc_cal[...] = part
        return carry

    lax.fori_loop(0, tiles // 2, bin_units, 0, unroll=6)
    mats_ref[...] = jnp.zeros_like(mats_ref)
    for block, at, h, start in block_pieces(blocks):
        mats_ref[block, 0:21, at : at + LANES] = acc_cal[
            h * UNIT_ROWS : h * UNIT_ROWS + 21, start : start + LANES
        ]
        if at == 0:
            for no, row in enumerate(global_rows):
                mats_ref[block, 21 + no : 22 + no, 0:LANES] = row

    def whole_copy(k):
        p = peer_tm(k)
        return pltpu.make_async_remote_copy(
            src_ref=mats_ref.at[lax.rem(p, blocks)],
            dst_ref=whole.at[t],
            send_sem=whole_s.at[k],
            recv_sem=whole_r.at[t],
            device_id={"tm": p, "grp": g},
            device_id_type=MESH,
        )

    def whole_arrival(k):
        p = peer_tm(k)
        return pltpu.make_async_remote_copy(
            src_ref=mats_ref.at[lax.rem(p, blocks)],
            dst_ref=whole.at[p],
            send_sem=whole_s.at[k],
            recv_sem=whole_r.at[p],
            device_id={"tm": p, "grp": g},
            device_id_type=MESH,
        )

    lax.fori_loop(1, count, lambda k, c: (whole_copy(k).start(), c)[1], 0)
    whole[t] = mats_ref[lax.rem(t, blocks)]
    near[groups + g] = normal_ref[...]

    @pl.when(jnp.logical_not(has_before))
    def _():
        near[0:groups] = jnp.zeros((groups, NORMAL_ROWS, LANES), F32)

    @pl.when(jnp.logical_not(has_after))
    def _():
        near[2 * groups :] = jnp.zeros((groups, NORMAL_ROWS, LANES), F32)

    each_near(lambda offset, k: near_arrival(offset, k).wait_recv())
    sums = []
    for s in range(3):
        part = near[s * groups]
        for q in range(1, groups):
            part = part + near[s * groups + q]
        sums.append(part)
    lane = lax.broadcasted_iota(jnp.int32, (NORMAL_ROWS, LANES), 1)
    before = pltpu.roll(sums[0], (HALO - nodes_dev) % LANES, 1)
    own = pltpu.roll(sums[1], HALO, 1)
    after = pltpu.roll(sums[2], (HALO + nodes_dev) % LANES, 1)
    end = nodes_dev + HALO
    normals = (
        own
        + jnp.where((lane >= 3) & (lane < HALO + 3), before, 0.0)
        + jnp.where((lane >= end) & (lane < end + HALO), after, 0.0)
    )
    spot = lax.broadcasted_iota(jnp.int32, (1, LANES), 1)
    exists = (spot >= jnp.where(has_before, 0, HALO)) & (
        spot < jnp.where(has_after, LANES, end)
    )
    normals = jnp.where(exists, normals, 0.0)
    index = {}
    for position, (a, b) in enumerate(pairs_of(3)):
        index[a, b] = index[b, a] = position
    band = [[normals[d * 6 + p : d * 6 + p + 1, :] for p in range(6)] for d in range(4)]
    right = [normals[24 + c : 25 + c, :] for c in range(3)]
    lower, inverse = cholesky_lists(symmetric(band[0], 3), 3)

    def precondition(vector):
        return solve_upper(lower, inverse, solve_lower(lower, inverse, vector))

    x = [OMEGA * value for value in precondition(right)]
    for _ in range(1, ATT_SWEEPS):
        out = [right[c] - x[c] for c in range(3)]
        for d in range(4):
            ahead = [pltpu.roll(x[c], LANES - d, 1) for c in range(3)] if d else x
            for a in range(3):
                for b in range(3):
                    out[a] = out[a] - band[d][index[a, b]] * ahead[b]
        for d in range(1, 4):
            for a in range(3):
                term = band[d][index[a, 0]] * x[0]
                for b in range(1, 3):
                    term = term + band[d][index[a, b]] * x[b]
                out[a] = out[a] - pltpu.roll(term, d, 1)
        change = precondition(out)
        x = [jnp.where(exists, x[c] + OMEGA * change[c], 0.0) for c in range(3)]
    for c in range(3):
        scaled = lower[c][c] * x[c]
        for k in range(c + 1, 3):
            scaled = scaled + lower[k][c] * x[k]
        moved = pltpu.roll(scaled, LANES - HALO, 1)
        step_ref[c : c + 1, :] = moved[:, 0:nodes_dev]


    local = kn_ref[...] - base + HALO
    tables = [jnp.broadcast_to(x[c], (tiles, LANES)) for c in range(3)]
    second = first
    for i in range(4):
        moved = ap_ref[0] * lane_pick(tables[0], local + i)
        for c in range(1, 3):
            moved = moved + ap_ref[c] * lane_pick(tables[c], local + i)
        second = second - basis[i] * moved
    second_ref[...] = second
    weighted = weights * second
    for a in range(CPAR):
        rcal[a * tiles : (a + 1) * tiles, :] = weighted * cp_ref[a]
    rcal[CPAR * tiles :, :] = jnp.zeros(((8 - CPAR) * tiles, LANES), F32)
    sums = [jnp.sum(weighted * gp_ref[a], axis=0, keepdims=True) for a in range(GPAR)]
    acc_rhs[...] = jnp.zeros_like(acc_rhs)

    def bin_rhs(no, carry):
        tile = no * 2
        units = two_rows(ci_ref, tile)
        upper, lower = lax.shift_right_logical(units, 8), lax.bitwise_and(units, 255)
        pieces = [by_high(p, upper) for p in split_three(two_tiles(rcal, tile, 8, tiles))]
        lhs = jnp.concatenate(pieces, axis=0).astype(BF16)
        acc_rhs[...] = acc_rhs[...] + dot_nt(lhs, one_hot(lower, LOW))
        return carry

    lax.fori_loop(0, tiles // 2, bin_rhs, 0, unroll=6)
    rows = 8 * (UNITS // LOW)
    total = acc_rhs[0:rows, :] + acc_rhs[rows : 2 * rows, :] + acc_rhs[2 * rows : 3 * rows, :]
    lane = lax.broadcasted_iota(jnp.int32, (1, LANES), 1)
    folded = [row + pltpu.roll(row, LANES // 2, 1) for row in sums]
    packed = [jnp.where(lane < LANES // 2, folded[2 * k], folded[2 * k + 1]) for k in range(2)]
    if rhs_ref.shape[2] > LANES:
        rhs_ref[...] = jnp.zeros_like(rhs_ref)
    for block, at, h, start in block_pieces(blocks):
        rhs_ref[block, 0:CPAR, at : at + LANES] = total[
            h * 8 : h * 8 + CPAR, start : start + LANES
        ]
        if at == 0:
            for k in range(2):
                rhs_ref[block, CPAR + k : CPAR + k + 1, 0:LANES] = packed[k]

    width = rhs_ref.shape[2]
    block = lax.rem(t, blocks)
    family = t - block

    def rwhole_copy(k, slot):
        p = peer_tm(k)
        return pltpu.make_async_remote_copy(
            src_ref=rhs_ref.at[lax.rem(p, blocks)],
            dst_ref=rwhole.at[slot],
            send_sem=rwhole_s.at[k],
            recv_sem=rwhole_r.at[slot],
            device_id={"tm": p, "grp": g},
            device_id_type=MESH,
        )

    lax.fori_loop(1, count, lambda k, c: (rwhole_copy(k, t).start(), c)[1], 0)
    rwhole[t] = rhs_ref[block]
    lax.fori_loop(1, count, lambda k, c: (whole_arrival(k).wait_recv(), c)[1], 0)
    mine[g] = lax.fori_loop(1, count, lambda k, c: c + whole[k], whole[0])

    def mine_copy(k):
        return pltpu.make_async_remote_copy(
            src_ref=mine.at[g],
            dst_ref=mine.at[g],
            send_sem=mine_s.at[k],
            recv_sem=mine_r.at[g],
            device_id={"tm": t, "grp": peer_grp(k)},
            device_id_type=MESH,
        )

    def mine_arrival(k):
        q = peer_grp(k)
        return pltpu.make_async_remote_copy(
            src_ref=mine.at[q],
            dst_ref=mine.at[q],
            send_sem=mine_s.at[k],
            recv_sem=mine_r.at[q],
            device_id={"tm": t, "grp": q},
            device_id_type=MESH,
        )

    for k in range(1, groups):
        mine_copy(k).start()
    for k in range(1, groups):
        mine_arrival(k).wait_recv()
    total = mine[0]
    for q in range(1, groups):
        total = total + mine[q]
    unit_total = total
    matrix = [unit_total[p : p + 1, :] for p in range(21)]
    lower, inverse = cholesky_lists(symmetric(matrix, CPAR), CPAR)
    upper_g = [
        jnp.broadcast_to(
            jnp.sum(unit_total[21 + p : 22 + p, 0:LANES], axis=1, keepdims=True), (1, LANES)
        )
        for p in range(10)
    ]
    lower_g, inverse_g = cholesky_lists(symmetric(upper_g, GPAR), GPAR)
    lax.fori_loop(1, count, lambda k, c: (rwhole_copy(k, peer_tm(k)).wait_recv(), c)[1], 0)
    rmine[g] = lax.fori_loop(1, count, lambda k, c: c + rwhole[k], rwhole[0])

    def rmine_copy(k, slot):
        return pltpu.make_async_remote_copy(
            src_ref=rmine.at[slot],
            dst_ref=rmine.at[slot],
            send_sem=rmine_s.at[k],
            recv_sem=rmine_r.at[slot],
            device_id={"tm": t, "grp": peer_grp(k)},
            device_id_type=MESH,
        )

    for k in range(1, groups):
        rmine_copy(k, g).start()
    for k in range(1, groups):
        rmine_copy(k, peer_grp(k)).wait_recv()
    total = rmine[0]
    for q in range(1, groups):
        total = total + rmine[q]
    right = [total[c : c + 1, :] for c in range(CPAR)]
    white = solve_lower(lower, inverse, right)
    solved = solve_upper(lower, inverse, white)
    for c in range(CPAR):
        ready[c : c + 1, :] = white[c]
        ready[CPAR + c : CPAR + c + 1, :] = solved[c]
    ready[2 * CPAR :, :] = jnp.zeros((16 - 2 * CPAR, width), F32)

    def spread_copy(k, slot):
        return pltpu.make_async_remote_copy(
            src_ref=ready,
            dst_ref=spread.at[slot],
            send_sem=spread_s.at[k],
            recv_sem=spread_r.at[slot],
            device_id={"tm": family + lax.rem(block + k, blocks), "grp": g},
            device_id_type=MESH,
        )

    lax.fori_loop(1, blocks, lambda k, c: (spread_copy(k, block).start(), c)[1], 0)
    spread[block] = ready[...]
    lane = lax.broadcasted_iota(jnp.int32, (1, LANES), 1)
    right_g = []
    for c in range(GPAR):
        row = total[CPAR + c // 2 : CPAR + c // 2 + 1, 0:LANES]
        half = (lane < LANES // 2) if c % 2 == 0 else (lane >= LANES // 2)
        value = jnp.sum(jnp.where(half, row, 0.0), axis=1, keepdims=True)
        right_g.append(jnp.broadcast_to(value, (1, LANES)))
    white_g = solve_lower(lower_g, inverse_g, right_g)
    solved_g = solve_upper(lower_g, inverse_g, white_g)
    for c in range(GPAR):
        glob_ref[c : c + 1, :] = white_g[c]
        glob_ref[GPAR + c : GPAR + c + 1, :] = solved_g[c]
    lax.fori_loop(
        1,
        blocks,
        lambda k, c: (spread_copy(k, lax.rem(block + k, blocks)).wait_recv(), c)[1],
        0,
    )
    out_ref[...] = spread[...]
    lax.fori_loop(1, count, lambda k, c: (rwhole_copy(k, t).wait_send(), c)[1], 0)
    for k in range(1, groups):
        rmine_copy(k, g).wait_send()
    lax.fori_loop(1, blocks, lambda k, c: (spread_copy(k, block).wait_send(), c)[1], 0)
    for k in range(1, groups):
        mine_copy(k).wait_send()
    each_near(lambda offset, k: near_copy(offset, k).wait_send())
    lax.fori_loop(1, count, lambda k, c: (whole_copy(k).wait_send(), c)[1], 0)


def final_kernel(
    blocks, second_ref, solved_ref, glob_ref, att_ref, cp_ref, ci_ref, gp_ref,
    res_ref, att_out_ref, step_ref, glob_out_ref,
):
    att_out_ref[...] = att_ref[...]
    lane = lax.broadcasted_iota(jnp.int32, (1, LANES), 1)
    packed = jnp.zeros((1, LANES), F32)
    for c in range(GPAR):
        packed = jnp.where(lane == c, glob_ref[c : c + 1, :], packed)
    glob_out_ref[...] = packed[:, 0:GPAR]
    tiles = second_ref.shape[0]
    units = ci_ref[...]
    high, low = lax.shift_right_logical(units, 7), lax.bitwise_and(units, 127)
    picked = [jnp.zeros((tiles, LANES), F32) for _ in range(CPAR)]
    width = UNITS // blocks
    for row in range(UNITS // LANES):
        block, at = (row * LANES) // width, (row * LANES) % width
        here = high == row
        step_ref[:, row * LANES : (row + 1) * LANES] = solved_ref[block, 0:CPAR, at : at + LANES]
        for c in range(CPAR):
            line = solved_ref[block, CPAR + c : CPAR + c + 1, at : at + LANES]
            table = jnp.broadcast_to(line, (tiles, LANES))
            picked[c] = jnp.where(here, lane_pick(table, low), picked[c])
    out = second_ref[...]
    for c in range(CPAR):
        out = out - cp_ref[c] * picked[c]
    for c in range(GPAR):
        out = out - gp_ref[c] * glob_ref[GPAR + c : GPAR + c + 1, :]
    res_ref[...] = out


def per_device(
    shape, residual, weight, source_part, source_index, source_delta, attitude_part,
    spline_phase, knot_index, calib_part, calib_index, global_part,
):
    count, groups, blocks = shape
    row_count = residual.shape[-1]
    tiles = row_count // TILE
    nodes_dev = tiles * KPT
    width = UNITS // blocks

    def flat(value):
        return value.reshape(tiles, TILE)

    def deep(value):
        return value.reshape(value.shape[0], -1, LANES)

    weights, phase, knots, units = map(flat, (weight, spline_phase, knot_index, calib_index))
    axes, calib, glob = map(deep, (attitude_part, calib_part, global_part))

    def out(*dims):
        return jax.ShapeDtypeStruct(dims, F32)

    dma = pltpu.SemaphoreType.DMA
    second, attitude_step, solved, global_out = pl.pallas_call(
        functools.partial(step_kernel, shape, nodes_dev),
        out_shape=(
            out(tiles, LANES), out(3, nodes_dev), out(blocks, 16, width), out(2 * GPAR, LANES),
        ),
        scratch_shapes=[
            pltpu.VMEM((ATT_ROWS * tiles, LANES), F32),
            pltpu.VMEM((UNIT_ROWS * tiles, LANES), F32),
            pltpu.VMEM((8 * tiles, LANES), F32),
            pltpu.VMEM((ATT_ROWS, LANES), F32),
            pltpu.VMEM((UNIT_ROWS * (UNITS // LOW), LOW), F32),
            pltpu.VMEM((3 * 8 * (UNITS // LOW), LOW), F32),
            pltpu.VMEM((NORMAL_ROWS, LANES), F32),
            pltpu.VMEM((blocks, NORMAL_ROWS, width), F32),
            pltpu.VMEM((blocks, 8, width), F32),
            pltpu.VMEM((3 * groups, NORMAL_ROWS, LANES), F32),
            pltpu.VMEM((groups, NORMAL_ROWS, width), F32),
            pltpu.VMEM((count, NORMAL_ROWS, width), F32),
            pltpu.VMEM((count, 8, width), F32),
            pltpu.VMEM((groups, 8, width), F32),
            pltpu.VMEM((16, width), F32),
            pltpu.VMEM((blocks, 16, width), F32),
            dma((3 * groups,)), dma((3 * groups,)),
            dma((groups,)), dma((groups,)),
            dma((count,)), dma((count,)),
            dma((count,)), dma((count,)),
            dma((groups,)), dma((groups,)),
            dma((blocks,)), dma((blocks,)),
        ],
        in_specs=[pl.BlockSpec(memory_space=pltpu.VMEM)] * 11,
        compiler_params=pltpu.CompilerParams(collective_id=0, has_side_effects=True),
        name="step",
    )(
        flat(residual), weights, deep(source_part), flat(source_index), deep(source_delta),
        axes, phase, knots, calib, units, glob,
    )
    final, attitude_out, calib_step, global_step = pl.pallas_call(
        functools.partial(final_kernel, blocks),
        out_shape=(
            out(tiles, LANES), out(3, nodes_dev), out(CPAR, UNITS), out(1, GPAR),
        ),
        name="final",
    )(second, solved, global_out, attitude_step, calib, units, glob)
    return final.reshape(residual.shape), attitude_out, calib_step, global_step.reshape(GPAR)


def solution(mesh):
    count, groups = mesh.shape["tm"], mesh.shape["grp"]
    blocks = min(count, UNITS // LANES)
    return jax.shard_map(
        functools.partial(per_device, (count, groups, blocks)),
        mesh=mesh,
        in_specs=(
            P("tm", "grp", None),
            P("tm", "grp", None),
            P(None, "tm", "grp", None),
            P("tm", "grp", None),
            P(None, "tm", None),
            P(None, "tm", "grp", None),
            P("tm", "grp", None),
            P("tm", "grp", None),
            P(None, "tm", "grp", None),
            P("tm", "grp", None),
            P(None, "tm", "grp", None),
        ),
        out_specs=(P("tm", "grp", None), P(None, "tm"), P(), P()),
        check_vma=False,
    )
```
